32 devices in a mesh: rep: 1 (over z), dp: 32 (over x, y, core).
Axes of the slice: x: 4, y: 4, z: 1, core: 2. Of those that a mesh axis runs over, the one named last changes fastest.
The devices are a block of a 4x4x8 slice.
Arguments:
- x: bfloat16 [32, 2048, 768], P(('rep', 'dp'))
- dy: bfloat16 [32, 2048, 768], P(('rep', 'dp'))
- w_gate: bfloat16 [2, 768, 2048], replicated
- w_up: bfloat16 [2, 768, 2048], replicated
- w_down: bfloat16 [2, 2048, 768], replicated
- m_w_gate: float32 [2, 768, 2048], P(None, 'dp')
- m_w_up: float32 [2, 768, 2048], P(None, 'dp')
- m_w_down: float32 [2, 2048, 768], P(None, 'dp')
- v_w_gate: float32 [2, 768, 2048], P(None, 'dp')
- v_w_up: float32 [2, 768, 2048], P(None, 'dp')
- v_w_down: float32 [2, 2048, 768], P(None, 'dp')
Outputs:
- output 1: bfloat16 [2, 768, 2048], P('rep')
- output 2: bfloat16 [2, 768, 2048], P('rep')
- output 3: bfloat16 [2, 2048, 768], P('rep')
- output 4: float32 [2, 768, 2048], P('rep', 'dp')
- output 5: float32 [2, 768, 2048], P('rep', 'dp')
- output 6: float32 [2, 2048, 768], P('rep', 'dp')
- output 7: float32 [2, 768, 2048], P('rep', 'dp')
- output 8: float32 [2, 768, 2048], P('rep', 'dp')
- output 9: float32 [2, 2048, 768], P('rep', 'dp')
All inputs are finite; a program needn't handle non-finite values.
Results may differ from the reference program's by a relative error of at most 0.022.
Values are sent between devices in bfloat16 or wider.
A program may use at most 768 MiB of HBM per device.

```python
import jax
import jax.numpy as jnp
from jax import lax

SEQUENCES = 32
TOKENS = 2048
D = 768
FF = 2048
LAYERS = 2
NAMES = ("w_gate", "w_up", "w_down")
SHAPES = {"w_gate": (LAYERS, D, FF), "w_up": (LAYERS, D, FF), "w_down": (LAYERS, FF, D)}


def bump(key, n, height):
    away = (jnp.arange(n, dtype=jnp.int32) - jax.random.randint(key, (), 0, n, jnp.int32)) % n
    return jnp.where(away < n // 8, height, 1.0)


def together(key, own, strength):
    shared = jax.random.normal(key, own.shape[1:], jnp.float32)
    return (own + strength * shared) * lax.rsqrt(1 + strength * strength)


def setup_inputs(seed: int = 0, part: int = 0) -> dict:
    kx, kdy, ka, kb, kz, kf, kh, kl, *keys = jax.random.split(jax.random.key(seed), 8 + 3 * len(NAMES))
    kx, kdy, ka, kb = (jax.random.fold_in(k, part) for k in (kx, kdy, ka, kb))
    kw, km, kv = (keys[i::3] for i in range(3))
    shape = (SEQUENCES, TOKENS, D)
    much_x, much_dy = jax.random.uniform(kz, (2,), jnp.float32, 0.0, 1.0)
    loud = 2.0 ** jax.random.uniform(jax.random.fold_in(kz, 1), (), jnp.float32, -1.0, 2.0)
    layers = 2.0 ** jax.random.uniform(kl, (LAYERS, 1, 1), jnp.float32, -1.0, 1.0)
    x = together(ka, jax.random.normal(kx, shape, jnp.float32), much_x) * bump(kf, D, 4.0)
    dy = together(kb, jax.random.normal(kdy, shape, jnp.float32), much_dy)
    drawn = {"x": x.astype(jnp.bfloat16), "dy": (loud * dy * (SEQUENCES * TOKENS) ** -0.5).astype(jnp.bfloat16)}
    for key, name in zip(kw, NAMES, strict=True):
        w = jax.random.normal(key, SHAPES[name], jnp.float32) * SHAPES[name][1] ** -0.5
        drawn[name] = (w * {"w_gate": 1.0, "w_up": bump(kh, FF, 4.0), "w_down": layers}[name]).astype(jnp.bfloat16)
    for key, name in zip(km, NAMES, strict=True):
        drawn[f"m_{name}"] = 0.1 * jax.random.normal(key, SHAPES[name], jnp.float32)
    for key, name in zip(kv, NAMES, strict=True):
        drawn[f"v_{name}"] = jax.random.uniform(key, SHAPES[name], jnp.float32, 0.005, 0.015)
    return drawn


def matmul(a, w):
    return jnp.dot(a, w, preferred_element_type=jnp.float32).astype(jnp.bfloat16)


def normed(h):
    wide = h.astype(jnp.float32)
    scale = lax.rsqrt(jnp.mean(wide**2, -1, keepdims=True) + 1e-6)
    return (wide * scale).astype(jnp.bfloat16)


def layer(h, w):
    a = normed(h)
    gate = jnp.dot(a, w["w_gate"], preferred_element_type=jnp.float32)
    up = jnp.dot(a, w["w_up"], preferred_element_type=jnp.float32)
    return h + matmul((jax.nn.silu(gate) * up).astype(jnp.bfloat16), w["w_down"])


def adamw(w, m, v, g):
    m = 0.9 * m + 0.1 * g
    v = 0.95 * v + 0.05 * g * g
    step = m * lax.rsqrt(v + 1e-8) + 0.1 * w
    return (w - 0.02 * step).astype(jnp.bfloat16), m, v


def clipped(gradients, sum_of_squares, count):
    factor = jnp.minimum(1.0, 0.5 * lax.rsqrt(sum_of_squares / count + 1e-30))
    return [g * factor for g in gradients]


def stack(weights, h):
    return lax.scan(lambda h, w: (layer(h, w), None), h, weights)[0]


def reference(x, dy, w_gate, w_up, w_down, m_w_gate, m_w_up, m_w_down, v_w_gate, v_w_up, v_w_down):
    weights = dict(zip(NAMES, (w_gate, w_up, w_down), strict=True))

    def take(so_far, sequence):
        h, by_y = sequence
        _, back = jax.vjp(lambda w: stack(w, h), weights)
        return jax.tree.map(lambda total, term: total + term.astype(jnp.float32), so_far, back(by_y)[0]), None

    none_yet = {name: jnp.zeros(w.shape, jnp.float32) for name, w in weights.items()}
    by_weights, _ = lax.scan(take, none_yet, (x, dy))
    gradients = [by_weights[name].astype(jnp.bfloat16).astype(jnp.float32) for name in NAMES]
    gradients = clipped(gradients, sum(jnp.sum(g * g) for g in gradients), sum(g.size for g in gradients))
    new = [
        adamw(w.astype(jnp.float32), m, v, g)
        for w, m, v, g in zip((w_gate, w_up, w_down), (m_w_gate, m_w_up, m_w_down), (v_w_gate, v_w_up, v_w_down), gradients, strict=True)
    ]
    return tuple(one[which] for which in range(3) for one in new)
```

```python
import functools
import math

import jax
import jax.numpy as jnp
from jax import lax
from jax.experimental import pallas as pl
from jax.experimental.pallas import tpu as pltpu
from jax.sharding import PartitionSpec as P

NAMES = ("w_gate", "w_up", "w_down")
F32, BF16 = jnp.float32, jnp.bfloat16
ANY = pl.BlockSpec(memory_space=pl.ANY)
VM = pl.BlockSpec(memory_space=pltpu.VMEM)
CORES = 2


def matmul(a, w):
    return jnp.dot(a, w, preferred_element_type=jnp.float32).astype(jnp.bfloat16)


def normed(h):
    wide = h.astype(jnp.float32)
    scale = lax.rsqrt(jnp.mean(wide**2, -1, keepdims=True) + 1e-6)
    return (wide * scale).astype(jnp.bfloat16)


def layer(h, w):
    a = normed(h)
    gate = jnp.dot(a, w["w_gate"], preferred_element_type=jnp.float32)
    up = jnp.dot(a, w["w_up"], preferred_element_type=jnp.float32)
    return h + matmul((jax.nn.silu(gate) * up).astype(jnp.bfloat16), w["w_down"])


def stack(weights, h):
    for number in range(weights["w_gate"].shape[0]):
        h = layer(h, {name: w[number] for name, w in weights.items()})
    return h


class Place:
    def __init__(self, n):
        self.n, self.side = n, math.isqrt(n // CORES)
        side = self.side
        me = lax.axis_index("dp")
        chip = lax.div(me, CORES)
        self.me = me
        self.core = lax.rem(me, CORES)
        self.x, self.y = lax.div(chip, side), lax.rem(chip, side)
        self.xy = (self.x, self.y)
        self.sibling = me + 1 - 2 * self.core

    def at(self, axis, step):
        return lax.rem(self.xy[axis] + step, self.side)

    def device(self, axis, step):
        to = list(self.xy)
        to[axis] = self.at(axis, step)
        return (to[0] * self.side + to[1]) * CORES + self.core


def chunk(color, p, q):
    return (p, q) if color == 0 else (q, p)


def tail_kernel(n, slabs, count, *refs):
    place = Place(n)
    side = place.side
    ns = len(slabs)
    g_in, w_in, m_in, v_in = (refs[i : i + 3] for i in (0, 3, 6, 9))
    w_out, m_out, v_out = (refs[i : i + 3] for i in (12, 15, 18))
    refs = refs[21:]
    per = {}
    for name in ("own", "d2d", "g", "wo", "mo", "vo", "nw"):
        per[name], refs = refs[:ns], refs[ns:]
    pbuf, refs = refs[:ns], refs[ns:]
    qbuf, refs = refs[:ns], refs[ns:]
    ssq, ssq_in, s_send, s_recv, a_send, a_recv, lsem, tsem_s, tsem_r, losem = refs
    last = side - 1

    def remote(src, dst, send, recv, device):
        return pltpu.make_async_remote_copy(
            src_ref=src, dst_ref=dst, send_sem=send, recv_sem=recv,
            device_id={"dp": device}, device_id_type=pl.DeviceIdType.MESH,
        )

    barrier = pltpu.get_barrier_semaphore()
    partners = [place.sibling] + [place.device(a, s) for a in (0, 1) for s in range(1, side)]
    for d in partners:
        pl.semaphore_signal(barrier, inc=1, device_id={"dp": d}, device_id_type=pl.DeviceIdType.MESH)

    local = []
    for s, (k, l, r, c) in enumerate(slabs):
        cp = pltpu.make_async_copy(g_in[k].at[l, :, :, place.core], per["own"][s], lsem.at[s, 0])
        cp.start()
        local.append([cp])
    pl.semaphore_wait(barrier, len(partners))
    d2d = []
    for s, (k, l, r, c) in enumerate(slabs):
        cp = remote(g_in[k].at[l, :, :, 1 - place.core], per["d2d"][s], s_send.at[s, 0, 7], s_recv.at[s, 0, 7], place.sibling)
        cp.start()
        d2d.append(cp)
    for s, (k, l, r, c) in enumerate(slabs):
        for j, (src, name) in enumerate(((w_in, "wo"), (m_in, "mo"), (v_in, "vo"))):
            view = src[k].at[l, place.x, place.y, place.core] if j == 0 else src[k].at[l]
            cp = pltpu.make_async_copy(view, per[name][s], lsem.at[s, 1 + j])
            cp.start()
            local[s].append(cp)

    pend = {}

    def send(s, c, slot, src, dst, device):
        cp = remote(src, dst, s_send.at[s, c, slot], s_recv.at[s, c, slot], device)
        cp.start()
        pend[s, c, slot] = cp

    def cols(s, c):
        half = slabs[s][3] // 2
        return pl.ds(c * half, half)

    def term(s, c, p, q):
        i, j = chunk(c, p, q)
        here = (i, j, slice(None), cols(s, c))
        return per["own"][s][here].astype(F32) + per["d2d"][s][here].astype(F32)

    def st1(s):
        local[s][0].wait()
        d2d[s].wait_recv()
        for c in (0, 1):
            b = pbuf[s].at[c]
            opp = place.at(c, 2)
            for q in range(side):
                b[0, q] = term(s, c, opp, q).astype(BF16)
            h = side // 2
            send(s, c, 0, b.at[0, pl.ds(0, h)], b.at[3, pl.ds(0, h)], place.device(c, 1))
            send(s, c, 1, b.at[0, pl.ds(h, h)], b.at[3, pl.ds(h, h)], place.device(c, last))

    def st2(s):
        h = side // 2
        for c in (0, 1):
            b = pbuf[s].at[c]
            pend[s, c, 0].wait_recv()
            for q in range(side):
                z = term(s, c, place.at(c, 1), q)
                b[1, q] = (z + b[3, q].astype(F32) if q < h else z).astype(BF16)
            send(s, c, 2, b.at[1], b.at[4], place.device(c, 1))
            pend[s, c, 1].wait_recv()
            for q in range(side):
                z = term(s, c, place.at(c, last), q)
                b[2, q] = (z + b[3, q].astype(F32) if q >= h else z).astype(BF16)
            send(s, c, 3, b.at[2], b.at[5], place.device(c, last))

    def psum(s, c, q):
        b = pbuf[s].at[c]
        return term(s, c, place.xy[c], q) + b[4, q].astype(F32) + b[5, q].astype(F32)

    def way(s):
        return 1 if s % 2 == 0 else last

    def st3(s):
        for c in (0, 1):
            pend[s, c, 2].wait_recv()
            pend[s, c, 3].wait_recv()
            b = qbuf[s].at[c]
            b[0] = psum(s, c, place.at(1 - c, 2)).astype(BF16)
            send(s, c, 4, b.at[0], b.at[3], place.device(1 - c, way(s)))

    def st4(s):
        for c in (0, 1):
            b = qbuf[s].at[c]
            pend[s, c, 4].wait_recv()
            for slot, step, to in ((1, 1, 4), (2, last, 5)):
                z = psum(s, c, place.at(1 - c, step))
                b[slot] = (z + b[3].astype(F32) if step == way(s) else z).astype(BF16)
                send(s, c, 4 + slot, b.at[slot], b.at[to], place.device(1 - c, step))

    def st5(s):
        rows, columns = slabs[s][2:]
        for c in (0, 1):
            b = qbuf[s].at[c]
            pend[s, c, 5].wait_recv()
            pend[s, c, 6].wait_recv()
            z = psum(s, c, place.xy[1 - c]) + b[4].astype(F32) + b[5].astype(F32)
            z = z.astype(BF16).astype(F32)
            per["g"][s][:, cols(s, c)] = z
            sq = z * z
            tot = None
            for i in range(0, rows, 8):
                for j in range(0, columns // 2, 128):
                    t = sq[i : i + 8, j : j + 128]
                    tot = t if tot is None else tot + t
            ssq[0] = tot if (s, c) == (0, 0) else ssq[0] + tot

    stages = (st1, st2, st3, st4, st5)
    for t in range(ns + len(stages) - 1):
        for i, st in enumerate(stages):
            if 0 <= t - i < ns:
                st(t - i)

    sends = []
    slot = 0
    for axis in (None, 0, 1):
        steps = (0,) if axis is None else range(1, side)
        mine = []
        for st in steps:
            device = place.sibling if axis is None else place.device(axis, st)
            cp = remote(ssq.at[0 if axis is None else axis + 1], ssq_in.at[slot], tsem_s.at[slot], tsem_r.at[slot], device)
            cp.start()
            mine.append((cp, slot))
            sends.append(cp)
            slot += 1
        z = ssq[0 if axis is None else axis + 1]
        for cp, sl in mine:
            cp.wait_recv()
            z = z + ssq_in[sl]
        ssq[1 if axis is None else axis + 2] = z
    total = jnp.sum(ssq[3], axis=(0, 1), keepdims=True)
    factor = jnp.minimum(1.0, 0.5 * lax.rsqrt(total / count + 1e-30))

    apend = {}

    def asend(s, c, slot, src, dst, device):
        cp = remote(src, dst, a_send.at[s, c, slot], a_recv.at[s, c, slot], device)
        cp.start()
        apend[s, c, slot] = cp

    def spot(s, c, p, q):
        k, l = slabs[s][:2]
        i, j = chunk(c, p, q)
        return w_out[k].at[l, i, j, place.core, :, cols(s, c)]

    outs = []

    def a0(s):
        k, l, rows, columns = slabs[s]
        for cp in local[s][1:]:
            cp.wait()
        for i in range(0, rows, 8):
            here = (pl.ds(i, 8), slice(None))
            g = per["g"][s][here] * factor
            m = 0.9 * per["mo"][s][here] + 0.1 * g
            v = 0.95 * per["vo"][s][here] + 0.05 * g * g
            w = per["wo"][s][here].astype(F32)
            step = m * lax.rsqrt(v + 1e-8) + 0.1 * w
            per["mo"][s][here] = m
            per["vo"][s][here] = v
            per["nw"][s][here] = (w - 0.02 * step).astype(BF16)
        for j, (src, dst) in enumerate(((per["nw"], w_out[k].at[l, place.x, place.y, place.core]), (per["mo"], m_out[k].at[l]), (per["vo"], v_out[k].at[l]))):
            cp = pltpu.make_async_copy(src[s], dst, losem.at[s, j])
            cp.start()
            outs.append(cp) if j else local[s].append(cp)
        for c in (0, 1):
            p, q = place.xy[c], place.xy[1 - c]
            mine = per["nw"][s].at[:, cols(s, c)]
            asend(s, c, 0, mine, spot(s, c, p, q), place.device(1 - c, 1))
            asend(s, c, 1, mine, spot(s, c, p, q), place.device(1 - c, last))

    def a1(s):
        step = way(s)
        for c in (0, 1):
            apend[s, c, 0].wait_recv()
            apend[s, c, 1].wait_recv()
            block = spot(s, c, place.xy[c], place.at(1 - c, side - step))
            asend(s, c, 2, block, block, place.device(1 - c, step))

    def a2(s):
        local[s][-1].wait()
        for c in (0, 1):
            apend[s, c, 2].wait_recv()
            row = spot(s, c, place.xy[c], slice(None))
            asend(s, c, 3, row, row, place.device(c, 1))
            asend(s, c, 4, row, row, place.device(c, last))
            asend(s, c, 7, row, row, place.sibling)

    def a3(s):
        h = side // 2
        for c in (0, 1):
            apend[s, c, 3].wait_recv()
            left = spot(s, c, place.at(c, last), pl.ds(0, h))
            asend(s, c, 5, left, left, place.device(c, 1))
            apend[s, c, 4].wait_recv()
            right = spot(s, c, place.at(c, 1), pl.ds(h, h))
            asend(s, c, 6, right, right, place.device(c, last))
            for slot, step in ((8, last), (9, 1)):
                row = spot(s, c, place.at(c, step), slice(None))
                asend(s, c, slot, row, row, place.sibling)

    def a4(s):
        for c in (0, 1):
            apend[s, c, 5].wait_recv()
            apend[s, c, 6].wait_recv()
            row = spot(s, c, place.at(c, 2), slice(None))
            asend(s, c, 10, row, row, place.sibling)

    stages = (a0, a1, a2, a3, a4)
    for t in range(ns + len(stages) - 1):
        for i, st in enumerate(stages):
            if 0 <= t - i < ns:
                st(t - i)
    for s in range(ns):
        d2d[s].wait_send()
        for c in (0, 1):
            for slot in (7, 8, 9, 10):
                apend[s, c, slot].wait_recv()
    for cp in list(pend.values()) + sends + list(apend.values()):
        cp.wait_send()
    for cp in outs:
        cp.wait()


def tail(n, grads, weights, m, v):
    side = math.isqrt(n // CORES)
    layers = weights[0].shape[0]
    shapes = [(t.shape[1], t.shape[2]) for t in m]
    slabs = tuple((k, l, *shapes[k]) for l in reversed(range(layers)) for k in (2, 0, 1))
    split = lambda t, k: t.reshape(layers, side, side, CORES, *shapes[k])
    grads = [split(t, k) for k, t in enumerate(grads)]
    weights = [split(t, k) for k, t in enumerate(weights)]
    count = sum(layers * n * r * c for r, c in shapes)
    ns = len(slabs)
    sc = []
    for lead, dtype in (((side, side), BF16), ((side, side), BF16), ((), F32), ((), BF16), ((), F32), ((), F32), ((), BF16)):
        sc += [pltpu.VMEM((*lead, r, c), dtype) for _, _, r, c in slabs]
    sc += [pltpu.VMEM((2, 6, side, r, c // 2), BF16) for _, _, r, c in slabs]
    sc += [pltpu.VMEM((2, 6, r, c // 2), BF16) for _, _, r, c in slabs]
    small = 1 + 2 * (side - 1)
    sc += [
        pltpu.VMEM((4, 8, 128), F32),
        pltpu.VMEM((small, 8, 128), F32),
        pltpu.SemaphoreType.DMA((ns, 2, 8)),
        pltpu.SemaphoreType.DMA((ns, 2, 8)),
        pltpu.SemaphoreType.DMA((ns, 2, 11)),
        pltpu.SemaphoreType.DMA((ns, 2, 11)),
        pltpu.SemaphoreType.DMA((ns, 4)),
        pltpu.SemaphoreType.DMA((small,)),
        pltpu.SemaphoreType.DMA((small,)),
        pltpu.SemaphoreType.DMA((ns, 3)),
    ]
    out = [jax.ShapeDtypeStruct(t.shape, BF16) for t in weights]
    out += [jax.ShapeDtypeStruct(t.shape, F32) for t in (*m, *v)]
    got = pl.pallas_call(
        functools.partial(tail_kernel, n, slabs, count),
        out_shape=out,
        in_specs=[ANY] * 12,
        out_specs=[ANY] * 9,
        scratch_shapes=sc,
        compiler_params=pltpu.CompilerParams(collective_id=0, has_side_effects=True, vmem_limit_bytes=60 * 2**20),
        name="tail",
    )(*grads, *weights, *m, *v)
    new = [t.reshape(layers, -1, t.shape[-1]) for t in got[:3]]
    return (*new, *got[3:])


def solution(mesh):
    n = mesh.shape["dp"]

    def step(x, dy, *arrays):
        weights, m, v = (arrays[i : i + 3] for i in (0, 3, 6))
        _, back = jax.vjp(lambda w: stack(w, x[0]), dict(zip(NAMES, weights, strict=True)))
        by_weights = back(dy[0])[0]
        return tail(n, [by_weights[name] for name in NAMES], weights, m, v)

    seq, whole, rows = P(("rep", "dp")), P(), P(None, "dp")
    return jax.shard_map(
        step,
        mesh=mesh,
        in_specs=(seq, seq, *[whole] * 3, *[rows] * 6),
        out_specs=(*[P("rep")] * 3, *[P("rep", "dp")] * 6),
        check_vma=False,
    )
```

```python
import functools
import math

import jax
import jax.numpy as jnp
from jax import lax
from jax.experimental import pallas as pl
from jax.experimental.pallas import tpu as pltpu
from jax.sharding import PartitionSpec as P

NAMES = ("w_gate", "w_up", "w_down")
F32, BF16 = jnp.float32, jnp.bfloat16
ANY = pl.BlockSpec(memory_space=pl.ANY)
VM = pl.BlockSpec(memory_space=pltpu.VMEM)
CORES = 2
LAGS = (0, 2, 5, 9, 12, 15)


def contract(a, b, dims):
    return lax.dot_general(a, b, ((dims[:1], dims[1:]), ((), ())), preferred_element_type=F32)


def rms_scale(wide):
    return lax.rsqrt(jnp.mean(wide**2, -1, keepdims=True) + 1e-6)


def sigmoid(t):
    return 0.5 * jnp.tanh(0.5 * t) + 0.5


def states_kernel(steps, chunk_f, *refs):
    x, dy, *weights = refs[:5]
    big_out = refs[5:11]
    at0, at1, dh_out = refs[11:14]
    vw, gate0, up0, bufs, wsem, osem = refs[14], refs[15], refs[16], refs[17], refs[18], refs[19]
    t = pl.program_id(0)
    rows = x.shape[1]
    ff = gate0.shape[1]
    layers = weights[0].shape[0]

    def load(k, l):
        dst = vw[k].at[l]
        return pltpu.make_async_copy(weights[k].at[l], dst, wsem.at[k, l])

    @pl.when(t == 0)
    def _():
        for k in range(3):
            load(k, 0).start()

    def need(k, l):
        @pl.when(t == 0)
        def _():
            load(k, l).wait()

    def put(i, tile):
        return pltpu.make_async_copy(bufs.at[i], big_out[i].at[pl.ds(tile * rows, rows)], osem.at[i])

    def free(i):
        @pl.when(t > 0)
        def _():
            put(i, t - 1).wait()

    def parts():
        return [pl.ds(j, chunk_f) for j in range(0, ff, chunk_f)]

    def back(j, dp, g, u, to_gate, to_up):
        sig = sigmoid(g)
        silu = g * sig
        bufs[to_up, :, j] = (dp * silu).astype(BF16)
        bufs[to_gate, :, j] = (dp * u * (sig * (1.0 + g * (1.0 - sig)))).astype(BF16)
        return silu

    h0 = x[0]
    wide = h0.astype(F32)
    a0 = (wide * rms_scale(wide)).astype(BF16)
    at0[...] = a0.T
    need(0, 0)
    need(1, 0)

    @pl.when(t == 0)
    def _():
        for l in range(1, layers):
            for k in range(3):
                load(k, l).start()

    free(0)
    for j in parts():
        g = contract(a0, vw[0][0, :, j], (1, 0))
        u = contract(a0, vw[1][0, :, j], (1, 0))
        gate0[:, j] = g
        up0[:, j] = u
        bufs[0, :, j] = (g * sigmoid(g) * u).astype(BF16)
    put(0, t).start()
    need(2, 0)
    y = contract(bufs[0], vw[2][0], (1, 0)).astype(BF16)
    h1 = (wide + y.astype(F32)).astype(BF16)

    wide = h1.astype(F32)
    scale = rms_scale(wide)
    a1 = (wide * scale).astype(BF16)
    at1[...] = a1.T
    for k in range(3):
        need(k, 1)
    for i in (1, 2, 3):
        free(i)
    d = dy[0]
    for j in parts():
        g = contract(a1, vw[0][1, :, j], (1, 0))
        u = contract(a1, vw[1][1, :, j], (1, 0))
        dp = contract(d, vw[2][1, j, :], (1, 1)).astype(BF16).astype(F32)
        silu = back(j, dp, g, u, 2, 3)
        bufs[1, :, j] = (silu * u).astype(BF16)
    for i in (1, 2, 3):
        put(i, t).start()
    da = contract(bufs[2], vw[0][1], (1, 1)).astype(BF16).astype(F32)
    da = da + contract(bufs[3], vw[1][1], (1, 1)).astype(BF16).astype(F32)
    da = da.astype(BF16).astype(F32)
    inner = jnp.mean(da * wide, -1, keepdims=True)
    dwide = da * scale - wide * (scale * scale * scale * inner)
    dh = (d.astype(F32) + dwide.astype(BF16).astype(F32)).astype(BF16)
    dh_out[...] = dh

    for i in (4, 5):
        free(i)
    for j in parts():
        dp = contract(dh, vw[2][0, j, :], (1, 1)).astype(BF16).astype(F32)
        back(j, dp, gate0[:, j], up0[:, j], 4, 5)
    for i in (4, 5):
        put(i, t).start()

    @pl.when(t == steps - 1)
    def _():
        for i in range(6):
            put(i, t).wait()


def states_body(steps, chunk_f, *refs):
    vw = refs[14:17]
    states_kernel(steps, chunk_f, *refs[:14], vw, *refs[17:])


def states(x, dy, weights):
    _, tokens, d = x.shape
    ff = weights[0].shape[2]
    tile = min(512, tokens)
    steps = tokens // tile
    seq = pl.BlockSpec((1, tile, d), lambda i: (0, i, 0))
    across = pl.BlockSpec((d, tile), lambda i: (0, i))
    out = [jax.ShapeDtypeStruct((tokens, ff), BF16)] * 6
    out += [jax.ShapeDtypeStruct((d, tokens), BF16)] * 2 + [jax.ShapeDtypeStruct((tokens, d), BF16)]
    flops = 2 * tokens * d * ff * 9
    return pl.pallas_call(
        functools.partial(states_body, steps, min(512, ff)),
        grid=(steps,),
        out_shape=out,
        in_specs=[seq, seq, ANY, ANY, ANY],
        out_specs=[ANY] * 6 + [across, across, pl.BlockSpec((tile, d), lambda i: (i, 0))],
        scratch_shapes=[pltpu.VMEM(w.shape, BF16) for w in weights]
        + [
            pltpu.VMEM((tile, ff), F32),
            pltpu.VMEM((tile, ff), F32),
            pltpu.VMEM((6, tile, ff), BF16),
            pltpu.SemaphoreType.DMA((3, weights[0].shape[0])),
            pltpu.SemaphoreType.DMA((6,)),
        ],
        compiler_params=pltpu.CompilerParams(vmem_limit_bytes=63 * 2**20, dimension_semantics=("arbitrary",)),
        cost_estimate=pl.CostEstimate(flops=flops, bytes_accessed=100 * 2**20, transcendentals=0),
        name="states",
    )(x, dy, *weights)


class Place:
    def __init__(self, n):
        self.n, self.side = n, math.isqrt(n // CORES)
        side = self.side
        me = lax.axis_index("dp")
        chip = lax.div(me, CORES)
        self.me = me
        self.core = lax.rem(me, CORES)
        self.x, self.y = lax.div(chip, side), lax.rem(chip, side)
        self.xy = (self.x, self.y)
        self.sibling = me + 1 - 2 * self.core

    def at(self, axis, step):
        return lax.rem(self.xy[axis] + step, self.side)

    def device(self, axis, step):
        to = list(self.xy)
        to[axis] = self.at(axis, step)
        return (to[0] * self.side + to[1]) * CORES + self.core


def chunk(color, p, q):
    return (p, q) if color == 0 else (q, p)


def tail_kernel(n, slabs, count, *refs):
    place = Place(n)
    side = place.side
    ns = len(slabs)
    at_in, an_in = refs[0:2], refs[2:4]
    b_in = (refs[4:6], refs[6:8], refs[8:10])
    w_in, m_in, v_in = (refs[i : i + 3] for i in (10, 13, 16))
    w_out, m_out, v_out = (refs[i : i + 3] for i in (19, 22, 25))
    refs = refs[28:]
    per = {}
    for name in ("full", "d2d", "g", "wo", "mo", "vo", "nw", "pbuf", "qbuf"):
        per[name], refs = refs[:ns], refs[ns:]
    pbuf, qbuf = per["pbuf"], per["qbuf"]
    at, an, btile, ssq, ssq_in, s_send, s_recv, a_send, a_recv, lsem, tsem_s, tsem_r, losem, asem, bsem = refs
    last = side - 1

    def remote(src, dst, send, recv, device):
        return pltpu.make_async_remote_copy(
            src_ref=src, dst_ref=dst, send_sem=send, recv_sem=recv,
            device_id={"dp": device}, device_id_type=pl.DeviceIdType.MESH,
        )

    barrier = pltpu.get_barrier_semaphore()
    partners = [place.sibling] + [place.device(a, s) for a in (0, 1) for s in range(1, side)]
    for d in partners:
        pl.semaphore_signal(barrier, inc=1, device_id={"dp": d}, device_id_type=pl.DeviceIdType.MESH)

    tiles = side
    tile = btile.shape[2]
    slots = btile.shape[0]

    def fetch(s, i):
        k, l = slabs[s][:2]
        slot = (s * tiles + i) % slots if isinstance(i, int) else lax.rem(s * tiles + i, slots)
        return pltpu.make_async_copy(b_in[k][l].at[:, pl.ds(i * tile, tile)], btile.at[slot], bsem.at[slot])

    def load_a(kind, l):
        src, dst = ((an_in[l], an), (at_in[l], at))[kind]
        return pltpu.make_async_copy(src, dst, asem.at[kind])

    top = slabs[0][1]
    load_a(1, top).start()
    fetch(0, 0).start()
    fetch(0, 1).start()
    load_a(0, top).start()
    held = [None, None]
    ssq[0] = jnp.zeros_like(ssq[0])
    local = [[] for _ in range(ns)]
    for s, (k, l, r, c) in enumerate(slabs):
        for j, (src, name) in enumerate(((w_in, "wo"), (m_in, "mo"), (v_in, "vo"))):
            view = src[k].at[l, place.x, place.y, place.core] if j == 0 else src[k].at[l]
            cp = pltpu.make_async_copy(view, per[name][s], lsem.at[s, j])
            cp.start()
            local[s].append(cp)

    def items(s):
        return range(2 if slabs[s][0] == 2 else tiles)

    def cols(s, c):
        width = slabs[s][3] // len(items(s))
        return pl.ds(c * width, width)

    def spot_in(s, c, p, q):
        i, j = chunk(c % 2, p, q)
        return per["full"][s].at[i, j, place.core, :, cols(s, c)]

    def term(s, c, p, q):
        i, j = chunk(c % 2, p, q)
        return spot_in(s, c, p, q)[...].astype(F32) + per["d2d"][s][i, j, :, cols(s, c)].astype(F32)

    def way(s):
        return 1 if s % 2 == 0 else last

    def wire(s, c, slot):
        h = side // 2
        b, b2 = pbuf[s].at[c], qbuf[s].at[c]
        opp = place.at(c % 2, 2)
        if slot == 0:
            ends = spot_in(s, c, opp, pl.ds(0, h)), b.at[0, pl.ds(0, h)], place.device(c % 2, 1)
        elif slot == 1:
            ends = spot_in(s, c, opp, pl.ds(h, h)), b.at[0, pl.ds(h, h)], place.device(c % 2, last)
        elif slot in (2, 3):
            step = 1 if slot == 2 else last
            ends = spot_in(s, c, place.at(c % 2, step), slice(None)), b.at[slot - 1], place.device(c % 2, step)
        elif slot == 4:
            ends = b2.at[0], b2.at[3], place.device(1 - c % 2, way(s))
        elif slot in (5, 6):
            ends = b2.at[slot - 4], b2.at[slot - 1], place.device(1 - c % 2, 1 if slot == 5 else last)
        else:
            ends = per["full"][s].at[:, :, 1 - place.core, :, cols(s, c)], per["d2d"][s].at[:, :, :, cols(s, c)], place.sibling
        return remote(*ends[:2], s_send.at[s, c, slot], s_recv.at[s, c, slot], ends[2])

    def st0(s, c):
        wire(s, c, 7).start()

    def st1(s, c):
        wire(s, c, 7).wait_recv()
        b = pbuf[s].at[c]
        opp = place.at(c % 2, 2)
        for q in range(side):
            spot_in(s, c, opp, q)[...] = term(s, c, opp, q).astype(BF16)
        h = side // 2
        wire(s, c, 0).start()
        wire(s, c, 1).start()

    def st2(s, c):
        h = side // 2
        b = pbuf[s].at[c]
        for slot, step, lo in ((2, 1, 0), (3, last, h)):
            wire(s, c, slot - 2).wait_recv()
            to = place.at(c % 2, step)
            for q in range(side):
                z = term(s, c, to, q)
                z = z + b[0, q].astype(F32) if lo <= q < lo + h else z
                spot_in(s, c, to, q)[...] = z.astype(BF16)
            wire(s, c, slot).start()

    def psum(s, c, q):
        b = pbuf[s].at[c]
        return term(s, c, place.xy[c % 2], q) + b[1, q].astype(F32) + b[2, q].astype(F32)

    def st3(s, c):
        wire(s, c, 2).wait_recv()
        wire(s, c, 3).wait_recv()
        b = qbuf[s].at[c]
        b[0] = psum(s, c, place.at(1 - c % 2, 2)).astype(BF16)
        wire(s, c, 4).start()

    def st4(s, c):
        b = qbuf[s].at[c]
        wire(s, c, 4).wait_recv()
        for slot, step, to in ((1, 1, 4), (2, last, 5)):
            z = psum(s, c, place.at(1 - c % 2, step))
            b[slot] = (z + b[3].astype(F32) if step == way(s) else z).astype(BF16)
            wire(s, c, 4 + slot).start()

    def st5(s, c):
        rows, columns = slabs[s][2:]
        b = qbuf[s].at[c]
        wire(s, c, 5).wait_recv()
        wire(s, c, 6).wait_recv()
        z = psum(s, c, place.xy[1 - c % 2]) + b[4].astype(F32) + b[5].astype(F32)
        z = z.astype(BF16).astype(F32)
        per["g"][s][:, cols(s, c)] = z
        sq = z * z
        tot = None
        for i in range(0, rows, 8):
            for j in range(0, columns // len(items(s)), 128):
                part = sq[i : i + 8, j : j + 128]
                tot = part if tot is None else tot + part
        ssq[0] = ssq[0] + tot

    stages = (st0, st1, st2, st3, st4, st5)
    events = []
    for s, (k, l, r, columns) in enumerate(slabs):
        for c in items(s):
            ready = s * tiles + (tiles if k == 2 else c + 1)
            events += [(ready + LAGS[i], i, s, c) for i in range(len(stages))]
    events.sort()

    def run(time):
        for when, i, s, c in events:
            if when == time:
                stages[i](s, c)

    for s, (k, l, r, columns) in enumerate(slabs):
        if s == 0:
            pl.semaphore_wait(barrier, len(partners))
        run(s * tiles)
        kind = 0 if k == 2 else 1
        if held[kind] != l:
            load_a(kind, l).wait()
            held[kind] = l

        @pl.loop(0, tiles)
        def _(i, s=s, k=k, r=r, columns=columns):
            for other in range(1, tiles):
                if any(e[0] == s * tiles + other for e in events):
                    pl.when(i == other)(functools.partial(run, s * tiles + other))
            fetch(s, i).wait()

            @pl.when(i < tiles - 2)
            def _():
                fetch(s, i + 2).start()

            if s + 1 < ns:

                @pl.when(i >= tiles - 2)
                def _():
                    fetch(s + 1, i - (tiles - 2)).start()

            slot = (s * tiles + i) % slots if isinstance(i, int) else lax.rem(s * tiles + i, slots)
            if k == 2:
                z = contract(btile[slot], an[...], (0, 0))
                per["full"][s][i] = z.reshape(side, CORES, r, columns).astype(BF16)
            else:
                z = contract(at[...], btile[slot], (1, 0))
                z = z.reshape(side, side, CORES, r, tile).astype(BF16)
                per["full"][s][:, :, :, :, pl.ds(pl.multiple_of(i * tile, tile), tile)] = z

        if l > 0 and not any((k2 == 2) == (k == 2) and l2 == l for k2, l2, _, _ in slabs[s + 1 :]):
            load_a(kind, l - 1).start()
    for time in range(ns * tiles, events[-1][0] + 1):
        run(time)

    sends = []
    slot = 0
    for axis in (None, 0, 1):
        steps = (0,) if axis is None else range(1, side)
        mine = []
        for st in steps:
            device = place.sibling if axis is None else place.device(axis, st)
            cp = remote(ssq.at[0 if axis is None else axis + 1], ssq_in.at[slot], tsem_s.at[slot], tsem_r.at[slot], device)
            cp.start()
            mine.append((cp, slot))
            sends.append(cp)
            slot += 1
        z = ssq[0 if axis is None else axis + 1]
        for cp, sl in mine:
            cp.wait_recv()
            z = z + ssq_in[sl]
        ssq[1 if axis is None else axis + 2] = z
    total = jnp.sum(ssq[3], axis=(0, 1), keepdims=True)
    factor = jnp.minimum(1.0, 0.5 * lax.rsqrt(total / count + 1e-30))

    apend = {}

    def asend(s, c, slot, src, dst, device):
        cp = remote(src, dst, a_send.at[s, c, slot], a_recv.at[s, c, slot], device)
        cp.start()
        apend[s, c, slot] = cp

    def half(s, c):
        width = slabs[s][3] // 2
        return pl.ds(c * width, width)

    def spot(s, c, p, q):
        k, l = slabs[s][:2]
        i, j = chunk(c, p, q)
        return w_out[k].at[l, i, j, place.core, :, half(s, c)]

    outs = []

    def a0(s):
        k, l, rows, columns = slabs[s]
        for cp in local[s]:
            cp.wait()
        for i in range(0, rows, 8):
            here = (pl.ds(i, 8), slice(None))
            g = per["g"][s][here] * factor
            m = 0.9 * per["mo"][s][here] + 0.1 * g
            v = 0.95 * per["vo"][s][here] + 0.05 * g * g
            w = per["wo"][s][here].astype(F32)
            step = m * lax.rsqrt(v + 1e-8) + 0.1 * w
            per["mo"][s][here] = m
            per["vo"][s][here] = v
            per["nw"][s][here] = (w - 0.02 * step).astype(BF16)
        for j, (src, dst) in enumerate(((per["nw"], w_out[k].at[l, place.x, place.y, place.core]), (per["mo"], m_out[k].at[l]), (per["vo"], v_out[k].at[l]))):
            cp = pltpu.make_async_copy(src[s], dst, losem.at[s, j])
            cp.start()
            outs.append(cp) if j else local[s].append(cp)
        for c in (0, 1):
            p, q = place.xy[c], place.xy[1 - c]
            mine = per["nw"][s].at[:, half(s, c)]
            asend(s, c, 0, mine, spot(s, c, p, q), place.device(1 - c, 1))
            asend(s, c, 1, mine, spot(s, c, p, q), place.device(1 - c, last))

    def a1(s):
        step = way(s)
        for c in (0, 1):
            apend[s, c, 0].wait_recv()
            apend[s, c, 1].wait_recv()
            block = spot(s, c, place.xy[c], place.at(1 - c, side - step))
            asend(s, c, 2, block, block, place.device(1 - c, step))

    def a2(s):
        local[s][-1].wait()
        for c in (0, 1):
            apend[s, c, 2].wait_recv()
            row = spot(s, c, place.xy[c], slice(None))
            asend(s, c, 3, row, row, place.device(c, 1))
            asend(s, c, 4, row, row, place.device(c, last))
            asend(s, c, 7, row, row, place.sibling)

    def a3(s):
        h = side // 2
        for c in (0, 1):
            apend[s, c, 3].wait_recv()
            left = spot(s, c, place.at(c, last), pl.ds(0, h))
            asend(s, c, 5, left, left, place.device(c, 1))
            apend[s, c, 4].wait_recv()
            right = spot(s, c, place.at(c, 1), pl.ds(h, h))
            asend(s, c, 6, right, right, place.device(c, last))
            for slot, step in ((8, last), (9, 1)):
                row = spot(s, c, place.at(c, step), slice(None))
                asend(s, c, slot, row, row, place.sibling)

    def a4(s):
        for c in (0, 1):
            apend[s, c, 5].wait_recv()
            apend[s, c, 6].wait_recv()
            row = spot(s, c, place.at(c, 2), slice(None))
            asend(s, c, 10, row, row, place.sibling)

    stages = (a0, a1, a2, a3, a4)
    for t in range(ns + len(stages) - 1):
        for i, st in enumerate(stages):
            if 0 <= t - i < ns:
                st(t - i)
    for s in range(ns):
        for c in (0, 1):
            for slot in (7, 8, 9, 10):
                apend[s, c, slot].wait_recv()
    for s in range(ns):
        for c in items(s):
            for slot in range(8):
                wire(s, c, slot).wait_send()
    for cp in sends + list(apend.values()):
        cp.wait_send()
    for cp in outs:
        cp.wait()


def tail(n, normal, across, wide, weights, m, v):
    side = math.isqrt(n // CORES)
    layers = weights[0].shape[0]
    shapes = [(t.shape[1], t.shape[2]) for t in m]
    slabs = tuple((k, l, *shapes[k]) for l in reversed(range(layers)) for k in ((0, 1, 2) if l == layers - 1 else (2, 0, 1)))
    weights = [t.reshape(layers, side, side, CORES, *shapes[k]) for k, t in enumerate(weights)]
    count = sum(layers * n * r * c for r, c in shapes)
    ns = len(slabs)
    tokens, ff = wide[0].shape
    d = normal[0].shape[1]
    sc = []
    for lead, dtype in (((side, side, CORES), BF16), ((side, side), BF16), ((), F32), ((), BF16), ((), F32), ((), F32), ((), BF16)):
        sc += [pltpu.VMEM((*lead, r, c), dtype) for _, _, r, c in slabs]
    pieces = [2 if k == 2 else side for k, _, _, _ in slabs]
    sc += [pltpu.VMEM((i, 3, side, r, c // i), BF16) for i, (_, _, r, c) in zip(pieces, slabs)]
    sc += [pltpu.VMEM((i, 6, r, c // i), BF16) for i, (_, _, r, c) in zip(pieces, slabs)]
    small = 1 + 2 * (side - 1)
    sc += [
        pltpu.VMEM((d, tokens), BF16),
        pltpu.VMEM((tokens, d), BF16),
        pltpu.VMEM((3, tokens, ff // side), BF16),
        pltpu.VMEM((4, 8, 128), F32),
        pltpu.VMEM((small, 8, 128), F32),
        pltpu.SemaphoreType.DMA((ns, side, 8)),
        pltpu.SemaphoreType.DMA((ns, side, 8)),
        pltpu.SemaphoreType.DMA((ns, 2, 11)),
        pltpu.SemaphoreType.DMA((ns, 2, 11)),
        pltpu.SemaphoreType.DMA((ns, 3)),
        pltpu.SemaphoreType.DMA((small,)),
        pltpu.SemaphoreType.DMA((small,)),
        pltpu.SemaphoreType.DMA((ns, 3)),
        pltpu.SemaphoreType.DMA((2,)),
        pltpu.SemaphoreType.DMA((3,)),
    ]
    out = [jax.ShapeDtypeStruct(t.shape, BF16) for t in weights]
    out += [jax.ShapeDtypeStruct(t.shape, F32) for t in (*m, *v)]
    ins = (*across, *normal, *wide, *weights, *m, *v)
    got = pl.pallas_call(
        functools.partial(tail_kernel, n, slabs, count),
        out_shape=out,
        in_specs=[ANY] * len(ins),
        out_specs=[ANY] * 9,
        scratch_shapes=sc,
        compiler_params=pltpu.CompilerParams(collective_id=0, has_side_effects=True, vmem_limit_bytes=67043328),
        name="tail",
    )(*ins)
    new = [t.reshape(layers, -1, t.shape[-1]) for t in got[:3]]
    return (*new, *got[3:])


def solution(mesh):
    n = mesh.shape["dp"]

    def step(x, dy, *arrays):
        weights, m, v = (arrays[i : i + 3] for i in (0, 3, 6))
        act0, act1, dg1, du1, dg0, du0, at0, at1, dh = states(x, dy, weights)
        return tail(n, (dh, dy[0]), (at0, at1), (dg0, dg1, du0, du1, act0, act1), weights, m, v)

    seq, whole, rows = P(("rep", "dp")), P(), P(None, "dp")
    return jax.shard_map(
        step,
        mesh=mesh,
        in_specs=(seq, seq, *[whole] * 3, *[rows] * 6),
        out_specs=(*[P("rep")] * 3, *[P("rep", "dp")] * 6),
        check_vma=False,
    )
```

```python
import functools
import math

import jax
import jax.numpy as jnp
from jax import lax
from jax.experimental import pallas as pl
from jax.experimental.pallas import tpu as pltpu
from jax.sharding import PartitionSpec as P

NAMES = ("w_gate", "w_up", "w_down")
F32, BF16 = jnp.float32, jnp.bfloat16
ANY = pl.BlockSpec(memory_space=pl.ANY)
VM = pl.BlockSpec(memory_space=pltpu.VMEM)
CORES = 2
LAGS = (0, 2, 5, 9, 12, 15)


def contract(a, b, dims):
    return lax.dot_general(a, b, ((dims[:1], dims[1:]), ((), ())), preferred_element_type=F32)


def rms_scale(wide):
    return lax.rsqrt(jnp.mean(wide**2, -1, keepdims=True) + 1e-6)


def sigmoid(t):
    return 0.5 * jnp.tanh(0.5 * t) + 0.5


def states_kernel(steps, chunk_f, *refs):
    x, dy, *weights = refs[:5]
    big_out = refs[5:11]
    at0, at1, dh_out = refs[11:14]
    vw, gate0, up0, bufs, wsem, osem = refs[14], refs[15], refs[16], refs[17], refs[18], refs[19]
    t = pl.program_id(0)
    rows = x.shape[1]
    ff = gate0.shape[1]
    layers = weights[0].shape[0]

    def load(k, l):
        dst = vw[k].at[l]
        return pltpu.make_async_copy(weights[k].at[l], dst, wsem.at[k, l])

    @pl.when(t == 0)
    def _():
        for k in range(3):
            load(k, 0).start()

    def need(k, l):
        @pl.when(t == 0)
        def _():
            load(k, l).wait()

    def put(i, tile):
        return pltpu.make_async_copy(bufs.at[i], big_out[i].at[pl.ds(tile * rows, rows)], osem.at[i])

    def free(i):
        @pl.when(t > 0)
        def _():
            put(i, t - 1).wait()

    def parts():
        return [pl.ds(j, chunk_f) for j in range(0, ff, chunk_f)]

    def back(j, dp, g, u, to_gate, to_up):
        sig = sigmoid(g)
        silu = g * sig
        bufs[to_up, :, j] = (dp * silu).astype(BF16)
        bufs[to_gate, :, j] = (dp * u * (sig * (1.0 + g * (1.0 - sig)))).astype(BF16)
        return silu

    h0 = x[0]
    wide = h0.astype(F32)
    a0 = (wide * rms_scale(wide)).astype(BF16)
    at0[...] = a0.T
    need(0, 0)
    need(1, 0)

    @pl.when(t == 0)
    def _():
        for l in range(1, layers):
            for k in range(3):
                load(k, l).start()

    free(0)
    for j in parts():
        g = contract(a0, vw[0][0, :, j], (1, 0))
        u = contract(a0, vw[1][0, :, j], (1, 0))
        gate0[:, j] = g
        up0[:, j] = u
        bufs[0, :, j] = (g * sigmoid(g) * u).astype(BF16)
    put(0, t).start()
    need(2, 0)
    y = contract(bufs[0], vw[2][0], (1, 0)).astype(BF16)
    h1 = (wide + y.astype(F32)).astype(BF16)

    wide = h1.astype(F32)
    scale = rms_scale(wide)
    a1 = (wide * scale).astype(BF16)
    at1[...] = a1.T
    for k in range(3):
        need(k, 1)
    for i in (1, 2, 3):
        free(i)
    d = dy[0]
    for j in parts():
        g = contract(a1, vw[0][1, :, j], (1, 0))
        u = contract(a1, vw[1][1, :, j], (1, 0))
        dp = contract(d, vw[2][1, j, :], (1, 1)).astype(BF16).astype(F32)
        silu = back(j, dp, g, u, 2, 3)
        bufs[1, :, j] = (silu * u).astype(BF16)
    for i in (1, 2, 3):
        put(i, t).start()
    da = contract(bufs[2], vw[0][1], (1, 1)).astype(BF16).astype(F32)
    da = da + contract(bufs[3], vw[1][1], (1, 1)).astype(BF16).astype(F32)
    da = da.astype(BF16).astype(F32)
    inner = jnp.mean(da * wide, -1, keepdims=True)
    dwide = da * scale - wide * (scale * scale * scale * inner)
    dh = (d.astype(F32) + dwide.astype(BF16).astype(F32)).astype(BF16)
    dh_out[...] = dh

    for i in (4, 5):
        free(i)
    for j in parts():
        dp = contract(dh, vw[2][0, j, :], (1, 1)).astype(BF16).astype(F32)
        back(j, dp, gate0[:, j], up0[:, j], 4, 5)
    for i in (4, 5):
        put(i, t).start()

    @pl.when(t == steps - 1)
    def _():
        for i in range(6):
            put(i, t).wait()


def states_body(steps, chunk_f, *refs):
    vw = refs[14:17]
    states_kernel(steps, chunk_f, *refs[:14], vw, *refs[17:])


def states(x, dy, weights):
    _, tokens, d = x.shape
    ff = weights[0].shape[2]
    tile = min(512, tokens)
    steps = tokens // tile
    seq = pl.BlockSpec((1, tile, d), lambda i: (0, i, 0))
    across = pl.BlockSpec((d, tile), lambda i: (0, i))
    out = [jax.ShapeDtypeStruct((tokens, ff), BF16)] * 6
    out += [jax.ShapeDtypeStruct((d, tokens), BF16)] * 2 + [jax.ShapeDtypeStruct((tokens, d), BF16)]
    flops = 2 * tokens * d * ff * 9
    return pl.pallas_call(
        functools.partial(states_body, steps, min(512, ff)),
        grid=(steps,),
        out_shape=out,
        in_specs=[seq, seq, ANY, ANY, ANY],
        out_specs=[ANY] * 6 + [across, across, pl.BlockSpec((tile, d), lambda i: (i, 0))],
        scratch_shapes=[pltpu.VMEM(w.shape, BF16) for w in weights]
        + [
            pltpu.VMEM((tile, ff), F32),
            pltpu.VMEM((tile, ff), F32),
            pltpu.VMEM((6, tile, ff), BF16),
            pltpu.SemaphoreType.DMA((3, weights[0].shape[0])),
            pltpu.SemaphoreType.DMA((6,)),
        ],
        compiler_params=pltpu.CompilerParams(vmem_limit_bytes=63 * 2**20, dimension_semantics=("arbitrary",)),
        cost_estimate=pl.CostEstimate(flops=flops, bytes_accessed=100 * 2**20, transcendentals=0),
        name="states",
    )(x, dy, *weights)


class Place:
    def __init__(self, n):
        self.n, self.side = n, math.isqrt(n // CORES)
        side = self.side
        me = lax.axis_index("dp")
        chip = lax.div(me, CORES)
        self.me = me
        self.core = lax.rem(me, CORES)
        self.x, self.y = lax.div(chip, side), lax.rem(chip, side)
        self.xy = (self.x, self.y)
        self.sibling = me + 1 - 2 * self.core

    def at(self, axis, step):
        return lax.rem(self.xy[axis] + step, self.side)

    def device(self, axis, step):
        to = list(self.xy)
        to[axis] = self.at(axis, step)
        return (to[0] * self.side + to[1]) * CORES + self.core


def chunk(color, p, q):
    return (p, q) if color == 0 else (q, p)


def tail_kernel(n, slabs, count, *refs):
    place = Place(n)
    side = place.side
    ns = len(slabs)
    at_in, an_in = refs[0:2], refs[2:4]
    b_in = (refs[4:6], refs[6:8], refs[8:10])
    w_in, m_in, v_in = (refs[i : i + 3] for i in (10, 13, 16))
    w_out, m_out, v_out = (refs[i : i + 3] for i in (19, 22, 25))
    refs = refs[28:]
    per = {}
    for name in ("full", "d2d", "g", "wo", "mo", "vo", "nw", "pbuf", "qbuf"):
        per[name], refs = refs[:ns], refs[ns:]
    pbuf, qbuf = per["pbuf"], per["qbuf"]
    at, an, btile, ssq, ssq_in, s_send, s_recv, a_send, a_recv, lsem, tsem_s, tsem_r, losem, asem, bsem = refs
    last = side - 1

    def remote(src, dst, send, recv, device):
        return pltpu.make_async_remote_copy(
            src_ref=src, dst_ref=dst, send_sem=send, recv_sem=recv,
            device_id={"dp": device}, device_id_type=pl.DeviceIdType.MESH,
        )

    barrier = pltpu.get_barrier_semaphore()
    partners = [place.sibling] + [place.device(a, s) for a in (0, 1) for s in range(1, side)]
    for d in partners:
        pl.semaphore_signal(barrier, inc=1, device_id={"dp": d}, device_id_type=pl.DeviceIdType.MESH)

    tiles = side
    tile = btile.shape[2]
    slots = btile.shape[0]

    def fetch(s, i):
        k, l = slabs[s][:2]
        slot = (s * tiles + i) % slots if isinstance(i, int) else lax.rem(s * tiles + i, slots)
        return pltpu.make_async_copy(b_in[k][l].at[:, pl.ds(i * tile, tile)], btile.at[slot], bsem.at[slot])

    def load_a(kind, l):
        src, dst = ((an_in[l], an), (at_in[l], at))[kind]
        return pltpu.make_async_copy(src, dst, asem.at[kind])

    top = slabs[0][1]
    load_a(1, top).start()
    fetch(0, 0).start()
    fetch(0, 1).start()
    load_a(0, top).start()
    held = [None, None]
    ssq[0] = jnp.zeros_like(ssq[0])
    local = [[] for _ in range(ns)]
    for s, (k, l, r, c) in enumerate(slabs):
        for j, (src, name) in enumerate(((w_in, "wo"), (m_in, "mo"), (v_in, "vo"))):
            view = src[k].at[l, place.x, place.y, place.core] if j == 0 else src[k].at[l]
            cp = pltpu.make_async_copy(view, per[name][s], lsem.at[s, j])
            cp.start()
            local[s].append(cp)

    def items(s):
        return range(2 if slabs[s][0] == 2 else tiles)

    def cols(s, c):
        width = slabs[s][3] // len(items(s))
        return pl.ds(c * width, width)

    def spot_in(s, c, p, q):
        i, j = chunk(c % 2, p, q)
        return per["full"][s].at[i, j, place.core, :, cols(s, c)]

    def term(s, c, p, q):
        i, j = chunk(c % 2, p, q)
        return spot_in(s, c, p, q)[...].astype(F32) + per["d2d"][s][i, j, :, cols(s, c)].astype(F32)

    def way(s):
        return 1 if s % 2 == 0 else last

    def wire(s, c, slot):
        h = side // 2
        b, b2 = pbuf[s].at[c], qbuf[s].at[c]
        opp = place.at(c % 2, 2)
        if slot == 0:
            ends = spot_in(s, c, opp, pl.ds(0, h)), b.at[0, pl.ds(0, h)], place.device(c % 2, 1)
        elif slot == 1:
            ends = spot_in(s, c, opp, pl.ds(h, h)), b.at[0, pl.ds(h, h)], place.device(c % 2, last)
        elif slot in (2, 3):
            step = 1 if slot == 2 else last
            ends = spot_in(s, c, place.at(c % 2, step), slice(None)), b.at[slot - 1], place.device(c % 2, step)
        elif slot == 4:
            ends = b2.at[0], b2.at[3], place.device(1 - c % 2, way(s))
        elif slot in (5, 6):
            ends = b2.at[slot - 4], b2.at[slot - 1], place.device(1 - c % 2, 1 if slot == 5 else last)
        else:
            ends = per["full"][s].at[:, :, 1 - place.core, :, cols(s, c)], per["d2d"][s].at[:, :, :, cols(s, c)], place.sibling
        return remote(*ends[:2], s_send.at[s, c, slot], s_recv.at[s, c, slot], ends[2])

    def st0(s, c):
        wire(s, c, 7).start()

    def st1(s, c):
        wire(s, c, 7).wait_recv()
        b = pbuf[s].at[c]
        opp = place.at(c % 2, 2)

        @pl.loop(0, side)
        def _(q):
            spot_in(s, c, opp, q)[...] = term(s, c, opp, q).astype(BF16)

        h = side // 2
        wire(s, c, 0).start()
        wire(s, c, 1).start()

    def st2(s, c):
        h = side // 2
        b = pbuf[s].at[c]
        for slot, step, lo in ((2, 1, 0), (3, last, h)):
            wire(s, c, slot - 2).wait_recv()
            to = place.at(c % 2, step)

            @pl.loop(0, h)
            def _(q, to=to, lo=lo):
                z = term(s, c, to, lo + q) + b[0, lo + q].astype(F32)
                spot_in(s, c, to, lo + q)[...] = z.astype(BF16)
                spot_in(s, c, to, h - lo + q)[...] = term(s, c, to, h - lo + q).astype(BF16)

            wire(s, c, slot).start()

    def psum(s, c, q):
        b = pbuf[s].at[c]
        return term(s, c, place.xy[c % 2], q) + b[1, q].astype(F32) + b[2, q].astype(F32)

    def st3(s, c):
        wire(s, c, 2).wait_recv()
        wire(s, c, 3).wait_recv()
        b = qbuf[s].at[c]
        b[0] = psum(s, c, place.at(1 - c % 2, 2)).astype(BF16)
        wire(s, c, 4).start()

    def st4(s, c):
        b = qbuf[s].at[c]
        wire(s, c, 4).wait_recv()
        for slot, step, to in ((1, 1, 4), (2, last, 5)):
            z = psum(s, c, place.at(1 - c % 2, step))
            b[slot] = (z + b[3].astype(F32) if step == way(s) else z).astype(BF16)
            wire(s, c, 4 + slot).start()

    def st5(s, c):
        rows, columns = slabs[s][2:]
        b = qbuf[s].at[c]
        wire(s, c, 5).wait_recv()
        wire(s, c, 6).wait_recv()
        z = psum(s, c, place.xy[1 - c % 2]) + b[4].astype(F32) + b[5].astype(F32)
        z = z.astype(BF16).astype(F32)
        per["g"][s][:, cols(s, c)] = z
        sq = z * z
        tot = None
        for i in range(0, rows, 8):
            for j in range(0, columns // len(items(s)), 128):
                part = sq[i : i + 8, j : j + 128]
                tot = part if tot is None else tot + part
        ssq[0] = ssq[0] + tot

    stages = (st0, st1, st2, st3, st4, st5)
    events = []
    for s, (k, l, r, columns) in enumerate(slabs):
        for c in items(s):
            ready = s * tiles + (tiles if k == 2 else c + 1)
            events += [(ready + LAGS[i], i, s, c) for i in range(len(stages))]
    events.sort()

    def run(time):
        for when, i, s, c in events:
            if when == time:
                stages[i](s, c)

    for s, (k, l, r, columns) in enumerate(slabs):
        if s == 0:
            pl.semaphore_wait(barrier, len(partners))
        run(s * tiles)
        kind = 0 if k == 2 else 1
        if held[kind] != l:
            load_a(kind, l).wait()
            held[kind] = l

        @pl.loop(0, tiles)
        def _(i, s=s, k=k, r=r, columns=columns):
            for other in range(1, tiles):
                if any(e[0] == s * tiles + other for e in events):
                    pl.when(i == other)(functools.partial(run, s * tiles + other))
            fetch(s, i).wait()

            @pl.when(i < tiles - 2)
            def _():
                fetch(s, i + 2).start()

            if s + 1 < ns:

                @pl.when(i >= tiles - 2)
                def _():
                    fetch(s + 1, i - (tiles - 2)).start()

            slot = (s * tiles + i) % slots if isinstance(i, int) else lax.rem(s * tiles + i, slots)
            if k == 2:
                z = contract(btile[slot], an[...], (0, 0))
                per["full"][s][i] = z.reshape(side, CORES, r, columns).astype(BF16)
            else:
                z = contract(at[...], btile[slot], (1, 0))
                z = z.reshape(side, side, CORES, r, tile).astype(BF16)
                per["full"][s][:, :, :, :, pl.ds(pl.multiple_of(i * tile, tile), tile)] = z

        if l > 0 and not any((k2 == 2) == (k == 2) and l2 == l for k2, l2, _, _ in slabs[s + 1 :]):
            load_a(kind, l - 1).start()
    for time in range(ns * tiles, events[-1][0] + 1):
        run(time)

    sends = []
    slot = 0
    for axis in (None, 0, 1):
        steps = (0,) if axis is None else range(1, side)
        mine = []
        for st in steps:
            device = place.sibling if axis is None else place.device(axis, st)
            cp = remote(ssq.at[0 if axis is None else axis + 1], ssq_in.at[slot], tsem_s.at[slot], tsem_r.at[slot], device)
            cp.start()
            mine.append((cp, slot))
            sends.append(cp)
            slot += 1
        z = ssq[0 if axis is None else axis + 1]
        for cp, sl in mine:
            cp.wait_recv()
            z = z + ssq_in[sl]
        ssq[1 if axis is None else axis + 2] = z
    total = jnp.sum(ssq[3], axis=(0, 1), keepdims=True)
    factor = jnp.minimum(1.0, 0.5 * lax.rsqrt(total / count + 1e-30))

    apend = {}

    def asend(s, c, slot, src, dst, device):
        cp = remote(src, dst, a_send.at[s, c, slot], a_recv.at[s, c, slot], device)
        cp.start()
        apend[s, c, slot] = cp

    def half(s, c):
        width = slabs[s][3] // 2
        return pl.ds(c * width, width)

    def spot(s, c, p, q):
        k, l = slabs[s][:2]
        i, j = chunk(c, p, q)
        return w_out[k].at[l, i, j, place.core, :, half(s, c)]

    outs = []

    def a0(s):
        k, l, rows, columns = slabs[s]
        for cp in local[s]:
            cp.wait()
        for i in range(0, rows, 8):
            here = (pl.ds(i, 8), slice(None))
            g = per["g"][s][here] * factor
            m = 0.9 * per["mo"][s][here] + 0.1 * g
            v = 0.95 * per["vo"][s][here] + 0.05 * g * g
            w = per["wo"][s][here].astype(F32)
            step = m * lax.rsqrt(v + 1e-8) + 0.1 * w
            per["mo"][s][here] = m
            per["vo"][s][here] = v
            per["nw"][s][here] = (w - 0.02 * step).astype(BF16)
        for j, (src, dst) in enumerate(((per["nw"], w_out[k].at[l, place.x, place.y, place.core]), (per["mo"], m_out[k].at[l]), (per["vo"], v_out[k].at[l]))):
            cp = pltpu.make_async_copy(src[s], dst, losem.at[s, j])
            cp.start()
            outs.append(cp) if j else local[s].append(cp)
        for c in (0, 1):
            p, q = place.xy[c], place.xy[1 - c]
            mine = per["nw"][s].at[:, half(s, c)]
            asend(s, c, 0, mine, spot(s, c, p, q), place.device(1 - c, 1))
            asend(s, c, 1, mine, spot(s, c, p, q), place.device(1 - c, last))

    def a1(s):
        step = way(s)
        for c in (0, 1):
            apend[s, c, 0].wait_recv()
            apend[s, c, 1].wait_recv()
            block = spot(s, c, place.xy[c], place.at(1 - c, side - step))
            asend(s, c, 2, block, block, place.device(1 - c, step))

    def a2(s):
        local[s][-1].wait()
        for c in (0, 1):
            apend[s, c, 2].wait_recv()
            row = spot(s, c, place.xy[c], slice(None))
            asend(s, c, 3, row, row, place.device(c, 1))
            asend(s, c, 4, row, row, place.device(c, last))
            asend(s, c, 7, row, row, place.sibling)

    def a3(s):
        h = side // 2
        for c in (0, 1):
            apend[s, c, 3].wait_recv()
            left = spot(s, c, place.at(c, last), pl.ds(0, h))
            asend(s, c, 5, left, left, place.device(c, 1))
            apend[s, c, 4].wait_recv()
            right = spot(s, c, place.at(c, 1), pl.ds(h, h))
            asend(s, c, 6, right, right, place.device(c, last))
            for slot, step in ((8, last), (9, 1)):
                row = spot(s, c, place.at(c, step), slice(None))
                asend(s, c, slot, row, row, place.sibling)

    def a4(s):
        for c in (0, 1):
            apend[s, c, 5].wait_recv()
            apend[s, c, 6].wait_recv()
            row = spot(s, c, place.at(c, 2), slice(None))
            asend(s, c, 10, row, row, place.sibling)

    stages = (a0, a1, a2, a3, a4)
    for t in range(ns + len(stages) - 1):
        for i, st in enumerate(stages):
            if 0 <= t - i < ns:
                st(t - i)
    for s in range(ns):
        for c in (0, 1):
            for slot in (7, 8, 9, 10):
                apend[s, c, slot].wait_recv()
    for s in range(ns):
        for c in items(s):
            for slot in range(8):
                wire(s, c, slot).wait_send()
    for cp in sends + list(apend.values()):
        cp.wait_send()
    for cp in outs:
        cp.wait()


def tail(n, normal, across, wide, weights, m, v):
    side = math.isqrt(n // CORES)
    layers = weights[0].shape[0]
    shapes = [(t.shape[1], t.shape[2]) for t in m]
    slabs = tuple((k, l, *shapes[k]) for l in reversed(range(layers)) for k in ((0, 1, 2) if l == layers - 1 else (2, 0, 1)))
    weights = [t.reshape(layers, side, side, CORES, *shapes[k]) for k, t in enumerate(weights)]
    count = sum(layers * n * r * c for r, c in shapes)
    ns = len(slabs)
    tokens, ff = wide[0].shape
    d = normal[0].shape[1]
    sc = []
    for lead, dtype in (((side, side, CORES), BF16), ((side, side), BF16), ((), F32), ((), BF16), ((), F32), ((), F32), ((), BF16)):
        sc += [pltpu.VMEM((*lead, r, c), dtype) for _, _, r, c in slabs]
    pieces = [2 if k == 2 else side for k, _, _, _ in slabs]
    sc += [pltpu.VMEM((i, 3, side, r, c // i), BF16) for i, (_, _, r, c) in zip(pieces, slabs)]
    sc += [pltpu.VMEM((i, 6, r, c // i), BF16) for i, (_, _, r, c) in zip(pieces, slabs)]
    small = 1 + 2 * (side - 1)
    sc += [
        pltpu.VMEM((d, tokens), BF16),
        pltpu.VMEM((tokens, d), BF16),
        pltpu.VMEM((3, tokens, ff // side), BF16),
        pltpu.VMEM((4, 8, 128), F32),
        pltpu.VMEM((small, 8, 128), F32),
        pltpu.SemaphoreType.DMA((ns, side, 8)),
        pltpu.SemaphoreType.DMA((ns, side, 8)),
        pltpu.SemaphoreType.DMA((ns, 2, 11)),
        pltpu.SemaphoreType.DMA((ns, 2, 11)),
        pltpu.SemaphoreType.DMA((ns, 3)),
        pltpu.SemaphoreType.DMA((small,)),
        pltpu.SemaphoreType.DMA((small,)),
        pltpu.SemaphoreType.DMA((ns, 3)),
        pltpu.SemaphoreType.DMA((2,)),
        pltpu.SemaphoreType.DMA((3,)),
    ]
    out = [jax.ShapeDtypeStruct(t.shape, BF16) for t in weights]
    out += [jax.ShapeDtypeStruct(t.shape, F32) for t in (*m, *v)]
    ins = (*across, *normal, *wide, *weights, *m, *v)
    got = pl.pallas_call(
        functools.partial(tail_kernel, n, slabs, count),
        out_shape=out,
        in_specs=[ANY] * len(ins),
        out_specs=[ANY] * 9,
        scratch_shapes=sc,
        compiler_params=pltpu.CompilerParams(collective_id=0, has_side_effects=True, vmem_limit_bytes=67043328),
        name="tail",
    )(*ins)
    new = [t.reshape(layers, -1, t.shape[-1]) for t in got[:3]]
    return (*new, *got[3:])


def solution(mesh):
    n = mesh.shape["dp"]

    def step(x, dy, *arrays):
        weights, m, v = (arrays[i : i + 3] for i in (0, 3, 6))
        act0, act1, dg1, du1, dg0, du0, at0, at1, dh = states(x, dy, weights)
        return tail(n, (dh, dy[0]), (at0, at1), (dg0, dg1, du0, du1, act0, act1), weights, m, v)

    seq, whole, rows = P(("rep", "dp")), P(), P(None, "dp")
    return jax.shard_map(
        step,
        mesh=mesh,
        in_specs=(seq, seq, *[whole] * 3, *[rows] * 6),
        out_specs=(*[P("rep")] * 3, *[P("rep", "dp")] * 6),
        check_vma=False,
    )
```

```python
import functools
import math

import jax
import jax.numpy as jnp
from jax import lax
from jax.experimental import pallas as pl
from jax.experimental.pallas import tpu as pltpu
from jax.sharding import PartitionSpec as P

NAMES = ("w_gate", "w_up", "w_down")
F32, BF16 = jnp.float32, jnp.bfloat16
ANY = pl.BlockSpec(memory_space=pl.ANY)
VM = pl.BlockSpec(memory_space=pltpu.VMEM)
CORES = 2
LAGS = (0, 2, 5, 10, 13, 17)


def contract(a, b, dims):
    return lax.dot_general(a, b, ((dims[:1], dims[1:]), ((), ())), preferred_element_type=F32)


def rms_scale(wide):
    return lax.rsqrt(jnp.mean(wide**2, -1, keepdims=True) + 1e-6)


def sigmoid(t):
    return 0.5 * jnp.tanh(0.5 * t) + 0.5


def states_kernel(steps, chunk_f, *refs):
    x, dy, *weights = refs[:5]
    big_out = refs[5:11]
    at0, at1, dh_out = refs[11:14]
    vw, gate0, up0, bufs, wsem, osem = refs[14], refs[15], refs[16], refs[17], refs[18], refs[19]
    t = pl.program_id(0)
    rows = x.shape[1]
    ff = gate0.shape[1]
    layers = weights[0].shape[0]

    def load(k, l):
        dst = vw[k].at[l]
        return pltpu.make_async_copy(weights[k].at[l], dst, wsem.at[k, l])

    @pl.when(t == 0)
    def _():
        for k in range(3):
            load(k, 0).start()

    def need(k, l):
        @pl.when(t == 0)
        def _():
            load(k, l).wait()

    def put(i, tile):
        return pltpu.make_async_copy(bufs.at[i], big_out[i].at[pl.ds(tile * rows, rows)], osem.at[i])

    def free(i):
        @pl.when(t > 0)
        def _():
            put(i, t - 1).wait()

    def parts():
        return [pl.ds(j, chunk_f) for j in range(0, ff, chunk_f)]

    def back(j, dp, g, u, to_gate, to_up):
        sig = sigmoid(g)
        silu = g * sig
        bufs[to_up, :, j] = (dp * silu).astype(BF16)
        bufs[to_gate, :, j] = (dp * u * (sig * (1.0 + g * (1.0 - sig)))).astype(BF16)
        return silu

    h0 = x[0]
    wide = h0.astype(F32)
    a0 = (wide * rms_scale(wide)).astype(BF16)
    at0[...] = a0.T
    need(0, 0)
    need(1, 0)

    @pl.when(t == 0)
    def _():
        for l in range(1, layers):
            for k in range(3):
                load(k, l).start()

    free(0)
    for j in parts():
        g = contract(a0, vw[0][0, :, j], (1, 0))
        u = contract(a0, vw[1][0, :, j], (1, 0))
        gate0[:, j] = g
        up0[:, j] = u
        bufs[0, :, j] = (g * sigmoid(g) * u).astype(BF16)
    put(0, t).start()
    need(2, 0)
    y = contract(bufs[0], vw[2][0], (1, 0)).astype(BF16)
    h1 = (wide + y.astype(F32)).astype(BF16)

    wide = h1.astype(F32)
    scale = rms_scale(wide)
    a1 = (wide * scale).astype(BF16)
    at1[...] = a1.T
    for k in range(3):
        need(k, 1)
    for i in (1, 2, 3):
        free(i)
    d = dy[0]
    for j in parts():
        g = contract(a1, vw[0][1, :, j], (1, 0))
        u = contract(a1, vw[1][1, :, j], (1, 0))
        dp = contract(d, vw[2][1, j, :], (1, 1)).astype(BF16).astype(F32)
        silu = back(j, dp, g, u, 2, 3)
        bufs[1, :, j] = (silu * u).astype(BF16)
    for i in (1, 2, 3):
        put(i, t).start()
    da = contract(bufs[2], vw[0][1], (1, 1)).astype(BF16).astype(F32)
    da = da + contract(bufs[3], vw[1][1], (1, 1)).astype(BF16).astype(F32)
    da = da.astype(BF16).astype(F32)
    inner = jnp.mean(da * wide, -1, keepdims=True)
    dwide = da * scale - wide * (scale * scale * scale * inner)
    dh = (d.astype(F32) + dwide.astype(BF16).astype(F32)).astype(BF16)
    dh_out[...] = dh

    for i in (4, 5):
        free(i)
    for j in parts():
        dp = contract(dh, vw[2][0, j, :], (1, 1)).astype(BF16).astype(F32)
        back(j, dp, gate0[:, j], up0[:, j], 4, 5)
    for i in (4, 5):
        put(i, t).start()

    @pl.when(t == steps - 1)
    def _():
        for i in range(6):
            put(i, t).wait()


def states_body(steps, chunk_f, *refs):
    vw = refs[14:17]
    states_kernel(steps, chunk_f, *refs[:14], vw, *refs[17:])


def states(x, dy, weights):
    _, tokens, d = x.shape
    ff = weights[0].shape[2]
    tile = min(512, tokens)
    steps = tokens // tile
    seq = pl.BlockSpec((1, tile, d), lambda i: (0, i, 0))
    across = pl.BlockSpec((d, tile), lambda i: (0, i))
    out = [jax.ShapeDtypeStruct((tokens, ff), BF16)] * 6
    out += [jax.ShapeDtypeStruct((d, tokens), BF16)] * 2 + [jax.ShapeDtypeStruct((tokens, d), BF16)]
    flops = 2 * tokens * d * ff * 9
    return pl.pallas_call(
        functools.partial(states_body, steps, min(512, ff)),
        grid=(steps,),
        out_shape=out,
        in_specs=[seq, seq, ANY, ANY, ANY],
        out_specs=[ANY] * 6 + [across, across, pl.BlockSpec((tile, d), lambda i: (i, 0))],
        scratch_shapes=[pltpu.VMEM(w.shape, BF16) for w in weights]
        + [
            pltpu.VMEM((tile, ff), F32),
            pltpu.VMEM((tile, ff), F32),
            pltpu.VMEM((6, tile, ff), BF16),
            pltpu.SemaphoreType.DMA((3, weights[0].shape[0])),
            pltpu.SemaphoreType.DMA((6,)),
        ],
        compiler_params=pltpu.CompilerParams(vmem_limit_bytes=63 * 2**20, dimension_semantics=("arbitrary",)),
        cost_estimate=pl.CostEstimate(flops=flops, bytes_accessed=100 * 2**20, transcendentals=0),
        name="states",
    )(x, dy, *weights)


class Place:
    def __init__(self, n):
        self.n, self.side = n, math.isqrt(n // CORES)
        side = self.side
        me = lax.axis_index("dp")
        chip = lax.div(me, CORES)
        self.me = me
        self.core = lax.rem(me, CORES)
        self.x, self.y = lax.div(chip, side), lax.rem(chip, side)
        self.xy = (self.x, self.y)
        self.sibling = me + 1 - 2 * self.core

    def at(self, axis, step):
        return lax.rem(self.xy[axis] + step, self.side)

    def device(self, axis, step):
        to = list(self.xy)
        to[axis] = self.at(axis, step)
        return (to[0] * self.side + to[1]) * CORES + self.core


def chunk(color, p, q):
    return (p, q) if color == 0 else (q, p)


def tail_kernel(n, slabs, count, *refs):
    place = Place(n)
    side = place.side
    ns = len(slabs)
    at_in, an_in = refs[0:2], refs[2:4]
    b_in = (refs[4:6], refs[6:8], refs[8:10])
    w_in, m_in, v_in = (refs[i : i + 3] for i in (10, 13, 16))
    w_out, m_out, v_out = (refs[i : i + 3] for i in (19, 22, 25))
    refs = refs[28:]
    per = {}
    for name in ("full", "d2d", "g", "wo", "mo", "vo", "nw", "pbuf", "qbuf"):
        per[name], refs = refs[:ns], refs[ns:]
    pbuf, qbuf = per["pbuf"], per["qbuf"]
    at, an, btile, ssq, ssq_in, s_send, s_recv, a_send, a_recv, lsem, tsem_s, tsem_r, losem, asem, bsem = refs
    last = side - 1

    def remote(src, dst, send, recv, device):
        return pltpu.make_async_remote_copy(
            src_ref=src, dst_ref=dst, send_sem=send, recv_sem=recv,
            device_id={"dp": device}, device_id_type=pl.DeviceIdType.MESH,
        )

    barrier = pltpu.get_barrier_semaphore()
    partners = [place.sibling] + [place.device(a, s) for a in (0, 1) for s in range(1, side)]
    for d in partners:
        pl.semaphore_signal(barrier, inc=1, device_id={"dp": d}, device_id_type=pl.DeviceIdType.MESH)

    tiles = side
    tile = btile.shape[2]
    slots = btile.shape[0]

    def fetch(s, i):
        k, l = slabs[s][:2]
        slot = (s * tiles + i) % slots if isinstance(i, int) else lax.rem(s * tiles + i, slots)
        return pltpu.make_async_copy(b_in[k][l].at[:, pl.ds(i * tile, tile)], btile.at[slot], bsem.at[slot])

    def load_a(kind, l):
        src, dst = ((an_in[l], an), (at_in[l], at))[kind]
        return pltpu.make_async_copy(src, dst, asem.at[kind])

    top = slabs[0][1]
    load_a(1, top).start()
    fetch(0, 0).start()
    fetch(0, 1).start()
    load_a(0, top).start()
    held = [None, None]
    ssq[0] = jnp.zeros_like(ssq[0])
    local = [[] for _ in range(ns)]
    for s, (k, l, r, c) in enumerate(slabs):
        for j, (src, name) in enumerate(((w_in, "wo"), (m_in, "mo"), (v_in, "vo"))):
            view = src[k].at[l, place.x, place.y, place.core] if j == 0 else src[k].at[l]
            cp = pltpu.make_async_copy(view, per[name][s], lsem.at[s, j])
            cp.start()
            local[s].append(cp)

    def items(s):
        return range(2 if slabs[s][0] == 2 else tiles)

    def cols(s, c):
        width = slabs[s][3] // len(items(s))
        return pl.ds(c * width, width)

    def spot_in(s, c, p, q):
        i, j = chunk(c % 2, p, q)
        return per["full"][s].at[i, j, place.core, :, cols(s, c)]

    def term(s, c, p, q):
        i, j = chunk(c % 2, p, q)
        return spot_in(s, c, p, q)[...].astype(F32) + per["d2d"][s][i, j, :, cols(s, c)].astype(F32)

    def way(s):
        return 1 if s % 2 == 0 else last

    def wire(s, c, slot):
        h = side // 2
        b, b2 = pbuf[s].at[c], qbuf[s].at[c]
        opp = place.at(c % 2, 2)
        if slot == 0:
            ends = spot_in(s, c, opp, pl.ds(0, h)), b.at[0, pl.ds(0, h)], place.device(c % 2, 1)
        elif slot == 1:
            ends = spot_in(s, c, opp, pl.ds(h, h)), b.at[0, pl.ds(h, h)], place.device(c % 2, last)
        elif slot in (2, 3):
            step = 1 if slot == 2 else last
            ends = spot_in(s, c, place.at(c % 2, step), slice(None)), b.at[slot - 1], place.device(c % 2, step)
        elif slot == 4:
            ends = b2.at[0], b2.at[3], place.device(1 - c % 2, way(s))
        elif slot in (5, 6):
            ends = b2.at[slot - 4], b2.at[slot - 1], place.device(1 - c % 2, 1 if slot == 5 else last)
        else:
            ends = per["full"][s].at[:, :, 1 - place.core, :, cols(s, c)], per["d2d"][s].at[:, :, :, cols(s, c)], place.sibling
        return remote(*ends[:2], s_send.at[s, c, slot], s_recv.at[s, c, slot], ends[2])

    def st0(s, c):
        wire(s, c, 7).start()

    def st1(s, c):
        wire(s, c, 7).wait_recv()
        b = pbuf[s].at[c]
        opp = place.at(c % 2, 2)

        @pl.loop(0, side)
        def _(q):
            spot_in(s, c, opp, q)[...] = term(s, c, opp, q).astype(BF16)

        h = side // 2
        wire(s, c, 0).start()
        wire(s, c, 1).start()

    def st2(s, c):
        h = side // 2
        b = pbuf[s].at[c]
        for slot, step, lo in ((2, 1, 0), (3, last, h)):
            wire(s, c, slot - 2).wait_recv()
            to = place.at(c % 2, step)

            @pl.loop(0, h)
            def _(q, to=to, lo=lo):
                z = term(s, c, to, lo + q) + b[0, lo + q].astype(F32)
                spot_in(s, c, to, lo + q)[...] = z.astype(BF16)
                spot_in(s, c, to, h - lo + q)[...] = term(s, c, to, h - lo + q).astype(BF16)

            wire(s, c, slot).start()

    def psum(s, c, q):
        b = pbuf[s].at[c]
        return term(s, c, place.xy[c % 2], q) + b[1, q].astype(F32) + b[2, q].astype(F32)

    def st3(s, c):
        wire(s, c, 2).wait_recv()
        wire(s, c, 3).wait_recv()
        b = qbuf[s].at[c]
        b[0] = psum(s, c, place.at(1 - c % 2, 2)).astype(BF16)
        wire(s, c, 4).start()

    def st4(s, c):
        b = qbuf[s].at[c]
        wire(s, c, 4).wait_recv()
        for slot, step, to in ((1, 1, 4), (2, last, 5)):
            z = psum(s, c, place.at(1 - c % 2, step))
            b[slot] = (z + b[3].astype(F32) if step == way(s) else z).astype(BF16)
            wire(s, c, 4 + slot).start()

    def st5(s, c):
        rows, columns = slabs[s][2:]
        b = qbuf[s].at[c]
        wire(s, c, 5).wait_recv()
        wire(s, c, 6).wait_recv()
        z = psum(s, c, place.xy[1 - c % 2]) + b[4].astype(F32) + b[5].astype(F32)
        z = z.astype(BF16).astype(F32)
        per["g"][s][:, cols(s, c)] = z
        sq = z * z
        tot = None
        for i in range(0, rows, 8):
            for j in range(0, columns // len(items(s)), 128):
                part = sq[i : i + 8, j : j + 128]
                tot = part if tot is None else tot + part
        ssq[0] = ssq[0] + tot

    stages = (st0, st1, st2, st3, st4, st5)
    events = []
    for s, (k, l, r, columns) in enumerate(slabs):
        for c in items(s):
            ready = s * tiles + (tiles if k == 2 else c + 1)
            events += [(ready + LAGS[i], i, s, c) for i in range(len(stages))]
    events.sort()

    def run(time):
        for when, i, s, c in events:
            if when == time:
                stages[i](s, c)

    for s, (k, l, r, columns) in enumerate(slabs):
        if s == 0:
            pl.semaphore_wait(barrier, len(partners))
        run(s * tiles)
        kind = 0 if k == 2 else 1
        if held[kind] != l:
            load_a(kind, l).wait()
            held[kind] = l

        @pl.loop(0, tiles)
        def _(i, s=s, k=k, r=r, columns=columns):
            for other in range(1, tiles):
                if any(e[0] == s * tiles + other for e in events):
                    pl.when(i == other)(functools.partial(run, s * tiles + other))
            fetch(s, i).wait()

            @pl.when(i < tiles - 2)
            def _():
                fetch(s, i + 2).start()

            if s + 1 < ns:

                @pl.when(i >= tiles - 2)
                def _():
                    fetch(s + 1, i - (tiles - 2)).start()

            slot = (s * tiles + i) % slots if isinstance(i, int) else lax.rem(s * tiles + i, slots)
            if k == 2:
                z = contract(btile[slot], an[...], (0, 0))
                per["full"][s][i] = z.reshape(side, CORES, r, columns).astype(BF16)
            else:
                z = contract(at[...], btile[slot], (1, 0))
                z = z.reshape(side, side, CORES, r, tile).astype(BF16)
                per["full"][s][:, :, :, :, pl.ds(pl.multiple_of(i * tile, tile), tile)] = z

        if l > 0 and not any((k2 == 2) == (k == 2) and l2 == l for k2, l2, _, _ in slabs[s + 1 :]):
            load_a(kind, l - 1).start()
    for time in range(ns * tiles, events[-1][0] + 1):
        run(time)

    sends = []
    slot = 0
    for axis in (None, 0, 1):
        steps = (0,) if axis is None else range(1, side)
        mine = []
        for st in steps:
            device = place.sibling if axis is None else place.device(axis, st)
            cp = remote(ssq.at[0 if axis is None else axis + 1], ssq_in.at[slot], tsem_s.at[slot], tsem_r.at[slot], device)
            cp.start()
            mine.append((cp, slot))
            sends.append(cp)
            slot += 1
        z = ssq[0 if axis is None else axis + 1]
        for cp, sl in mine:
            cp.wait_recv()
            z = z + ssq_in[sl]
        ssq[1 if axis is None else axis + 2] = z
    total = jnp.sum(ssq[3], axis=(0, 1), keepdims=True)
    factor = jnp.minimum(1.0, 0.5 * lax.rsqrt(total / count + 1e-30))

    apend = {}

    def asend(s, c, slot, src, dst, device):
        cp = remote(src, dst, a_send.at[s, c, slot], a_recv.at[s, c, slot], device)
        cp.start()
        apend[s, c, slot] = cp

    def half(s, c):
        width = slabs[s][3] // 2
        return pl.ds(c * width, width)

    def spot(s, c, p, q):
        k, l = slabs[s][:2]
        i, j = chunk(c, p, q)
        return w_out[k].at[l, i, j, place.core, :, half(s, c)]

    outs = []

    def a0(s):
        k, l, rows, columns = slabs[s]
        for cp in local[s]:
            cp.wait()
        for i in range(0, rows, 8):
            here = (pl.ds(i, 8), slice(None))
            g = per["g"][s][here] * factor
            m = 0.9 * per["mo"][s][here] + 0.1 * g
            v = 0.95 * per["vo"][s][here] + 0.05 * g * g
            w = per["wo"][s][here].astype(F32)
            step = m * lax.rsqrt(v + 1e-8) + 0.1 * w
            per["mo"][s][here] = m
            per["vo"][s][here] = v
            per["nw"][s][here] = (w - 0.02 * step).astype(BF16)
        for j, (src, dst) in enumerate(((per["nw"], w_out[k].at[l, place.x, place.y, place.core]), (per["mo"], m_out[k].at[l]), (per["vo"], v_out[k].at[l]))):
            cp = pltpu.make_async_copy(src[s], dst, losem.at[s, j])
            cp.start()
            outs.append(cp) if j else local[s].append(cp)
        for c in (0, 1):
            p, q = place.xy[c], place.xy[1 - c]
            mine = per["nw"][s].at[:, half(s, c)]
            asend(s, c, 0, mine, spot(s, c, p, q), place.device(1 - c, 1))
            asend(s, c, 1, mine, spot(s, c, p, q), place.device(1 - c, last))

    def a1(s):
        step = way(s)
        for c in (0, 1):
            apend[s, c, 0].wait_recv()
            apend[s, c, 1].wait_recv()
            block = spot(s, c, place.xy[c], place.at(1 - c, side - step))
            asend(s, c, 2, block, block, place.device(1 - c, step))

    def a2(s):
        local[s][-1].wait()
        for c in (0, 1):
            apend[s, c, 2].wait_recv()
            row = spot(s, c, place.xy[c], slice(None))
            asend(s, c, 3, row, row, place.device(c, 1))
            asend(s, c, 4, row, row, place.device(c, last))
            asend(s, c, 7, row, row, place.sibling)

    def a3(s):
        h = side // 2
        for c in (0, 1):
            apend[s, c, 3].wait_recv()
            left = spot(s, c, place.at(c, last), pl.ds(0, h))
            asend(s, c, 5, left, left, place.device(c, 1))
            apend[s, c, 4].wait_recv()
            right = spot(s, c, place.at(c, 1), pl.ds(h, h))
            asend(s, c, 6, right, right, place.device(c, last))
            for slot, step in ((8, last), (9, 1)):
                row = spot(s, c, place.at(c, step), slice(None))
                asend(s, c, slot, row, row, place.sibling)

    def a4(s):
        for c in (0, 1):
            apend[s, c, 5].wait_recv()
            apend[s, c, 6].wait_recv()
            row = spot(s, c, place.at(c, 2), slice(None))
            asend(s, c, 10, row, row, place.sibling)

    stages = (a0, a1, a2, a3, a4)
    for t in range(ns + len(stages) - 1):
        for i, st in enumerate(stages):
            if 0 <= t - i < ns:
                st(t - i)
    for s in range(ns):
        for c in (0, 1):
            for slot in (7, 8, 9, 10):
                apend[s, c, slot].wait_recv()
    for s in range(ns):
        for c in items(s):
            for slot in range(8):
                wire(s, c, slot).wait_send()
    for cp in sends + list(apend.values()):
        cp.wait_send()
    for cp in outs:
        cp.wait()


def tail(n, normal, across, wide, weights, m, v):
    side = math.isqrt(n // CORES)
    layers = weights[0].shape[0]
    shapes = [(t.shape[1], t.shape[2]) for t in m]
    slabs = tuple((k, l, *shapes[k]) for l in reversed(range(layers)) for k in ((0, 1, 2) if l == layers - 1 else (2, 0, 1)))
    weights = [t.reshape(layers, side, side, CORES, *shapes[k]) for k, t in enumerate(weights)]
    count = sum(layers * n * r * c for r, c in shapes)
    ns = len(slabs)
    tokens, ff = wide[0].shape
    d = normal[0].shape[1]
    sc = []
    for lead, dtype in (((side, side, CORES), BF16), ((side, side), BF16), ((), F32), ((), BF16), ((), F32), ((), F32), ((), BF16)):
        sc += [pltpu.VMEM((*lead, r, c), dtype) for _, _, r, c in slabs]
    pieces = [2 if k == 2 else side for k, _, _, _ in slabs]
    sc += [pltpu.VMEM((i, 3, side, r, c // i), BF16) for i, (_, _, r, c) in zip(pieces, slabs)]
    sc += [pltpu.VMEM((i, 6, r, c // i), BF16) for i, (_, _, r, c) in zip(pieces, slabs)]
    small = 1 + 2 * (side - 1)
    sc += [
        pltpu.VMEM((d, tokens), BF16),
        pltpu.VMEM((tokens, d), BF16),
        pltpu.VMEM((3, tokens, ff // side), BF16),
        pltpu.VMEM((4, 8, 128), F32),
        pltpu.VMEM((small, 8, 128), F32),
        pltpu.SemaphoreType.DMA((ns, side, 8)),
        pltpu.SemaphoreType.DMA((ns, side, 8)),
        pltpu.SemaphoreType.DMA((ns, 2, 11)),
        pltpu.SemaphoreType.DMA((ns, 2, 11)),
        pltpu.SemaphoreType.DMA((ns, 3)),
        pltpu.SemaphoreType.DMA((small,)),
        pltpu.SemaphoreType.DMA((small,)),
        pltpu.SemaphoreType.DMA((ns, 3)),
        pltpu.SemaphoreType.DMA((2,)),
        pltpu.SemaphoreType.DMA((3,)),
    ]
    out = [jax.ShapeDtypeStruct(t.shape, BF16) for t in weights]
    out += [jax.ShapeDtypeStruct(t.shape, F32) for t in (*m, *v)]
    ins = (*across, *normal, *wide, *weights, *m, *v)
    got = pl.pallas_call(
        functools.partial(tail_kernel, n, slabs, count),
        out_shape=out,
        in_specs=[ANY] * len(ins),
        out_specs=[ANY] * 9,
        scratch_shapes=sc,
        compiler_params=pltpu.CompilerParams(collective_id=0, has_side_effects=True, vmem_limit_bytes=67043328),
        name="tail",
    )(*ins)
    new = [t.reshape(layers, -1, t.shape[-1]) for t in got[:3]]
    return (*new, *got[3:])


def solution(mesh):
    n = mesh.shape["dp"]

    def step(x, dy, *arrays):
        weights, m, v = (arrays[i : i + 3] for i in (0, 3, 6))
        act0, act1, dg1, du1, dg0, du0, at0, at1, dh = states(x, dy, weights)
        return tail(n, (dh, dy[0]), (at0, at1), (dg0, dg1, du0, du1, act0, act1), weights, m, v)

    seq, whole, rows = P(("rep", "dp")), P(), P(None, "dp")
    return jax.shard_map(
        step,
        mesh=mesh,
        in_specs=(seq, seq, *[whole] * 3, *[rows] * 6),
        out_specs=(*[P("rep")] * 3, *[P("rep", "dp")] * 6),
        check_vma=False,
    )
```
